32 devices in a mesh: dp: 8 (over z, y), fsdp: 4 (over x, core).
Axes of the slice: x: 2, y: 2, z: 4, core: 2. Of those that a mesh axis runs over, the one named last changes fastest.
Arguments:
- tokens: bfloat16 [16384, 4096], P(('dp', 'fsdp')), may hold values from -0.75 to 0.75
- doc_ids: int32 [16384], P(('dp', 'fsdp')), may hold values from 0 to 15, never falling along the last dimension, each value on 1 to 2048 neighbouring positions
- attn_gain: float32 [4096], replicated, may hold values from 0.1 to 1.9
- mlp_gain: float32 [4096], replicated, may hold values from 0.1 to 1.9
- w_query: bfloat16 [4096, 512], P(('dp', 'fsdp')), may hold values from -1 to 1
- w_key_value: bfloat16 [4096, 256], P(('dp', 'fsdp')), may hold values from -3 to 3
- w_out: bfloat16 [512, 4096], P(None, ('dp', 'fsdp')), may hold values from -0.25 to 0.25
- w_gate: bfloat16 [4096, 1024], P(('dp', 'fsdp')), may hold values from -0.09375 to 0.09375
- w_up: bfloat16 [4096, 1024], P(('dp', 'fsdp')), may hold values from -0.09375 to 0.09375
- w_down: bfloat16 [1024, 4096], P(None, ('dp', 'fsdp')), may hold values from -0.1875 to 0.1875
Outputs:
- mixed: bfloat16 [16384, 4096], P(('dp', 'fsdp'))
The draws below stay inside these ranges and needn't reach their ends.
Inputs may be any that keep to these rules, and one draw needn't show every extreme that they name: `doc_ids`: document numbers never fall along the pack, and every document has at most 2048 tokens.
All inputs are finite; a program needn't handle non-finite values.
Results may differ from the reference program's by a relative error of at most 0.02.
The reference program's roundings to bfloat16 on the way count: a program that leaves them out, or rounds other values in their place, can miss the bound.
Values may be sent and summed in bfloat16 or wider, within the bound.
A program may use at most 128 MiB of HBM per device.

```python
import math
import jax
import jax.numpy as jnp
import numpy as np
from jax import lax

D = 4096
HQ = 4
HD = 128
FF = 1024
TOK_DEV = 512
HALO = 2048
TOKENS = 16384
DOCS = 16
N_DP = 8
N_FSDP = 4


def shared_query(key):
    base = jax.random.normal(jax.random.fold_in(key, 11), (D, HQ * HD), jnp.float32)
    return jnp.clip(base, -6.0, 6.0) / math.sqrt(D)


def draw_w_query(key, part):
    return shared_query(key).astype(jnp.bfloat16)


def draw_w_key_value(key, part):
    fresh = jax.random.normal(jax.random.fold_in(key, 23), (D, 2 * HD), jnp.float32)
    fresh = jnp.clip(fresh, -6.0, 6.0) / math.sqrt(D)
    return fresh.astype(jnp.bfloat16)


def block_levels(stream_key, extent, split, smallest, high):
    def one(dim, parts):
        steps = jax.random.uniform(jax.random.fold_in(jax.random.fold_in(stream_key, 6), dim), (parts,), jnp.float32, smallest / len(split), high / len(split))
        return jnp.repeat(jnp.exp(steps), extent[dim] // parts).reshape((-1,) + (1,) * (len(extent) - dim - 1))

    level = one(*split[0])
    for cut in split[1:]:
        level = level * one(*cut)
    return level


def split_up(count, total, most, slope):
    weights = [(1 << 20) // math.isqrt(grade ** slope) + 1 for grade in range(2, count + 1)]
    rest, holding = total - most - (count - 1), [1] * (count - 1)
    while rest > 0:
        movable = [i for i in range(count - 1) if holding[i] < most]
        whole, remaining = sum([weights[i] for i in movable]), rest
        for i in movable:
            addition = min(most - holding[i], max(1, remaining * weights[i] // whole), rest)
            holding[i] = holding[i] + addition
            rest = rest - addition
    return np.array([most] + holding)


def ragged_sizes(own_key, number_of, total, most, skew):
    if number_of == 2:
        one = jax.random.randint(own_key, (), max(1, total - most), min(most, total - 1) + 1)
        return jnp.stack([one, total - one])
    sizes = jnp.asarray(split_up(number_of, total, most, skew), jnp.int32)
    pairs = (number_of - 1) // 2
    donor, receiver = sizes[1:1 + 2 * pairs:2], sizes[2:2 + 2 * pairs:2]
    margin = jnp.minimum(donor - 1, most - receiver)
    passed = jax.random.randint(jax.random.fold_in(own_key, 1), (pairs,), 0, 1 << 20) % (margin + 1)
    sizes = sizes.at[1:1 + 2 * pairs:2].set(donor - passed).at[2:2 + 2 * pairs:2].set(receiver + passed)
    return sizes[jax.random.permutation(jax.random.fold_in(own_key, 2), number_of)]


def noise(stream_key, extent, spread, limit, shards=(), kind=jnp.bfloat16):
    values = spread * jax.random.normal(stream_key, extent, jnp.float32)
    if shards:
        values = values * block_levels(stream_key, extent, shards, -0.22, 0.18)
    return jnp.clip(values, -limit, limit).astype(kind)


def setup_inputs(seed: int = 0) -> dict:
    splits = jax.random.split(jax.random.key(seed), 11)
    return {
        "tokens": noise(splits[0], (TOKENS, D), 0.05, 0.75, ((0, 32),)),
        "doc_ids": jnp.searchsorted(jnp.cumsum(ragged_sizes(splits[1], DOCS, TOKENS, HALO, 1)), jnp.arange(TOKENS), side="right").astype(jnp.int32),
        "attn_gain": jnp.clip(1.0 + 0.18 * jax.random.normal(splits[2], (D,), jnp.float32), 0.1, 1.9),
        "mlp_gain": jnp.clip(1.0 + 0.18 * jax.random.normal(splits[3], (D,), jnp.float32), 0.1, 1.9),
        "w_query": draw_w_query(jax.random.fold_in(splits[10], 71), 0),
        "w_key_value": draw_w_key_value(jax.random.fold_in(splits[10], 71), 0),
        "w_out": noise(splits[6], (HQ * HD, D), (HQ * HD) ** -0.5, 0.25, ((1, 32),)),
        "w_gate": noise(splits[7], (D, FF), D ** -0.5, 0.09375, ((0, 32),)),
        "w_up": noise(splits[8], (D, FF), D ** -0.5, 0.09375, ((0, 32),)),
        "w_down": noise(splits[9], (FF, D), FF ** -0.5, 0.1875, ((1, 32),)),
    }


EPS = 1e-05
THETA = 500000.0
NEGATIVE = -1e+30

def rms_scale(values, gain):
    wide = values.astype(jnp.float32)
    power = lax.optimization_barrier(jnp.mean(wide * wide, axis=-1, keepdims=True))
    return (wide * lax.rsqrt(power + EPS) * gain).astype(jnp.bfloat16)

def rotate(values, position):
    head = values.shape[-1]
    half = head // 2
    freqs = THETA ** (-2.0 * jnp.arange(half, dtype=jnp.float32) / head)
    angle = position.astype(jnp.float32)[:, None, None] * freqs[None, None, :]
    cosine = jnp.cos(angle)
    sine = jnp.sin(angle)
    first = values[..., :half]
    second = values[..., half:]
    return jnp.concatenate([first * cosine - second * sine, second * cosine + first * sine], axis=-1)

def widen(values):
    return lax.optimization_barrier(values).astype(jnp.float32)

def attend(query, keys, values, key_marks, marks, offset):
    scores = jnp.einsum('qhd,kd->hqk', widen(query), widen(keys)) / math.sqrt(query.shape[-1])
    key_index = jnp.arange(keys.shape[0], dtype=jnp.int32)
    query_index = jnp.arange(query.shape[0], dtype=jnp.int32) + offset
    allowed = (key_marks[None, :] == marks[:, None]) & (key_index[None, :] <= query_index[:, None])
    scores = jnp.where(allowed[None, :, :], scores, NEGATIVE)
    peak = lax.optimization_barrier(jnp.max(scores, axis=2, keepdims=True))
    weights = jnp.exp(scores - peak)
    totals = lax.optimization_barrier(jnp.sum(weights, axis=2))
    mixed = jnp.einsum('hqk,kd->qhd', widen(weights.astype(jnp.bfloat16)), widen(values))
    return mixed / jnp.transpose(totals)[:, :, None]

def reference(tokens, doc_ids, attn_gain, mlp_gain, w_query, w_key_value, w_out, w_gate, w_up, w_down):
    total_rows = tokens.shape[0]
    normed = rms_scale(tokens, attn_gain)
    query_raw = jnp.dot(normed, w_query, preferred_element_type=jnp.float32)
    pair_raw = jnp.dot(normed, w_key_value, preferred_element_type=jnp.float32)
    position = jnp.arange(total_rows, dtype=jnp.int32)
    query = rotate(query_raw.reshape(total_rows, HQ, HD), position).astype(jnp.bfloat16)
    keys = rotate(pair_raw[:, None, :HD], position)[:, 0, :].astype(jnp.bfloat16)
    values = pair_raw[:, HD:].astype(jnp.bfloat16)
    marks = doc_ids + 1
    key_padded = jnp.concatenate([jnp.zeros((HALO, HD), jnp.bfloat16), keys], axis=0)
    value_padded = jnp.concatenate([jnp.zeros((HALO, HD), jnp.bfloat16), values], axis=0)
    mark_padded = jnp.concatenate([jnp.zeros((HALO,), jnp.int32), marks], axis=0)

    def one_rank(rank):
        start = (rank * TOK_DEV).astype(jnp.int32)
        rank_query = lax.dynamic_slice_in_dim(query, start, TOK_DEV, 0)
        rank_marks = lax.dynamic_slice_in_dim(marks, start, TOK_DEV, 0)
        rank_keys = lax.dynamic_slice_in_dim(key_padded, start, HALO + TOK_DEV, 0)
        rank_values = lax.dynamic_slice_in_dim(value_padded, start, HALO + TOK_DEV, 0)
        key_marks = lax.dynamic_slice_in_dim(mark_padded, start, HALO + TOK_DEV, 0)
        mixed = attend(rank_query, rank_keys, rank_values, key_marks, rank_marks, HALO)
        return mixed.reshape(TOK_DEV, HQ * HD).astype(jnp.bfloat16)
    attended = lax.map(one_rank, jnp.arange(N_DP * N_FSDP, dtype=jnp.int32)).reshape(total_rows, HQ * HD)
    projected = jnp.dot(attended, w_out, preferred_element_type=jnp.float32)
    resid = (tokens.astype(jnp.float32) + projected).astype(jnp.bfloat16)
    resid = lax.optimization_barrier(resid)
    normed_mlp = rms_scale(resid, mlp_gain)
    gate = jnp.dot(normed_mlp, w_gate, preferred_element_type=jnp.float32)
    up_value = jnp.dot(normed_mlp, w_up, preferred_element_type=jnp.float32)
    hidden = (jax.nn.silu(gate) * up_value).astype(jnp.bfloat16)
    down = jnp.dot(hidden, w_down, preferred_element_type=jnp.float32)
    return (resid.astype(jnp.float32) + down).astype(jnp.bfloat16)
```

```python
import functools
import math

import jax
import jax.numpy as jnp
from jax import lax
from jax.experimental import pallas as pl
from jax.experimental.pallas import tpu as pltpu
from jax.sharding import PartitionSpec as P

SPAN = 4


EPS = 1e-05
THETA = 500000.0
NEGATIVE = -1e30


def shifted(array, axis, by):
    length = lax.axis_size(axis)
    pairs = [(i, i + by) for i in range(length) if 0 <= i + by < length]
    return lax.ppermute(array, axis, pairs)


def rms_scale(values, gain):
    wide = values.astype(jnp.float32)
    power = jnp.mean(wide * wide, axis=-1, keepdims=True)
    return (wide * lax.rsqrt(power + EPS) * gain).astype(jnp.bfloat16)


def rotate(values, position):
    head = values.shape[-1]
    half = head // 2
    freqs = THETA ** (-2.0 * jnp.arange(half, dtype=jnp.float32) / head)
    angle = position.astype(jnp.float32)[:, None, None] * freqs[None, None, :]
    cosine = jnp.cos(angle)
    sine = jnp.sin(angle)
    first = values[..., :half]
    second = values[..., half:]
    return jnp.concatenate(
        [first * cosine - second * sine, second * cosine + first * sine], axis=-1
    )


def head_scores(query, keys):
    return jnp.einsum("qhd,kd->hqk", query, keys, preferred_element_type=jnp.float32) / math.sqrt(
        query.shape[-1]
    )


def weigh_values(weights, values):
    return jnp.einsum(
        "hqk,kd->qhd", weights.astype(jnp.bfloat16), values, preferred_element_type=jnp.float32
    )


def attend_dense(query, keys, values, key_marks, marks, offset):
    scores = head_scores(query, keys)
    key_index = jnp.arange(keys.shape[0], dtype=jnp.int32)
    query_index = jnp.arange(query.shape[0], dtype=jnp.int32) + offset
    allowed = (key_marks[None, :] == marks[:, None]) & (key_index[None, :] <= query_index[:, None])
    scores = jnp.where(allowed[None, :, :], scores, NEGATIVE)
    peak = jnp.max(scores, axis=2, keepdims=True)
    weights = jnp.exp(scores - peak)
    totals = jnp.sum(weights, axis=2)
    return weigh_values(weights, values) / jnp.transpose(totals)[:, :, None]


MESH = pl.DeviceIdType.MESH


class Gather:
    def __init__(self, spot, own, full, send, recv, local, row):
        self.own, self.full = own, full
        self.send, self.recv, self.local, self.row = send, recv, local, row
        self.dp, self.fsdp, self.depth = spot
        self.z, self.y = self.dp // 2, self.dp % 2
        self.x, self.c = self.fsdp // 2, self.fsdp % 2
        self.right = (self.dp, (1 - self.x) * 2 + self.c)
        self.up = (self.z * 2 + 1 - self.y, self.fsdp)
        self.twin = (self.dp, self.x * 2 + 1 - self.c)
        self.base = self.depth - 1

    def peers(self):
        others = [
            (lax.rem(self.z + step, self.depth) * 2 + self.y, self.fsdp)
            for step in range(1, self.depth)
        ]
        return others + [self.right, self.up, self.twin]

    def copy(self, number, source, target, device):
        return pltpu.make_async_remote_copy(
            src_ref=source,
            dst_ref=target,
            send_sem=self.send.at[self.row, number],
            recv_sem=self.recv.at[self.row, number],
            device_id=device,
            device_id_type=MESH,
        )

    def column(self, y, x, number, device, c=None):
        c = self.c if c is None else c
        part = self.full.at[:, y, x, c]
        return self.copy(number, part, part, device)

    def half(self, y, x, which, number, device):
        middle = self.depth // 2
        part = self.full.at[pl.ds(which * middle, middle), y, x, self.c]
        return self.copy(number, part, part, device)

    def mine(self):
        return pltpu.make_async_copy(
            self.own, self.full.at[self.z, self.y, self.x, self.c], self.local.at[self.row]
        )

    def along(self, step):
        there = (lax.rem(self.z + step, self.depth) * 2 + self.y, self.fsdp)
        return self.copy(
            step - 1, self.own, self.full.at[self.z, self.y, self.x, self.c], there
        )

    def s0(self):
        self.mine().start()
        for step in range(1, self.depth):
            self.along(step).start()

    def s1(self):
        self.mine().wait()
        for step in range(1, self.depth):
            self.along(step).wait_recv()
        self.column(self.y, self.x, self.base, self.right).start()
        self.column(self.y, self.x, self.base + 1, self.up).start()
        self.column(self.y, self.x, self.base + 4, self.twin).start()

    def s2(self):
        self.column(self.y, self.x, self.base, self.right).wait_recv()
        self.column(self.y, self.x, self.base + 1, self.up).wait_recv()
        self.half(1 - self.y, self.x, 0, self.base + 2, self.right).start()
        self.half(self.y, 1 - self.x, 1, self.base + 3, self.up).start()
        self.column(self.y, 1 - self.x, self.base + 5, self.twin).start()
        self.column(1 - self.y, self.x, self.base + 6, self.twin).start()

    def s3(self):
        self.half(1 - self.y, self.x, 0, self.base + 2, self.right).wait_recv()
        self.half(self.y, 1 - self.x, 1, self.base + 3, self.up).wait_recv()
        self.column(1 - self.y, 1 - self.x, self.base + 7, self.twin).start()

    def s4(self):
        for step in range(1, self.depth):
            self.along(step).wait_send()
        self.column(self.y, self.x, self.base, self.right).wait_send()
        self.column(self.y, self.x, self.base + 1, self.up).wait_send()
        self.half(1 - self.y, self.x, 0, self.base + 2, self.right).wait_send()
        self.half(self.y, 1 - self.x, 1, self.base + 3, self.up).wait_send()
        self.column(self.y, self.x, self.base + 4, self.twin).wait()
        self.column(self.y, 1 - self.x, self.base + 5, self.twin).wait()
        self.column(1 - self.y, self.x, self.base + 6, self.twin).wait()
        self.column(1 - self.y, 1 - self.x, self.base + 7, self.twin).wait()


def greet(peers):
    barrier = pltpu.get_barrier_semaphore()
    for device in peers:
        pl.semaphore_signal(barrier, inc=1, device_id=device, device_id_type=MESH)
    pl.semaphore_wait(barrier, len(peers))


def gather_kernel(depth, count, *refs):
    owns, fulls = refs[:count], refs[count : 2 * count]
    send, recv, local = refs[2 * count :]
    spot = (lax.axis_index("dp"), lax.axis_index("fsdp"), depth)
    rides = [Gather(spot, owns[i], fulls[i], send, recv, local, i) for i in range(count)]
    greet(rides[0].peers())
    for ride in rides:
        ride.s0()
    for slot in range(count + 3):
        for stage, lag in (("s1", 0), ("s2", 1), ("s3", 2), ("s4", 3)):
            if 0 <= slot - lag < count:
                getattr(rides[slot - lag], stage)()


def gather_all(arrays):
    depth = lax.axis_size("dp") // 2
    count = len(arrays)
    copies = depth - 1 + 8
    return pl.pallas_call(
        functools.partial(gather_kernel, depth, count),
        out_shape=[
            jax.ShapeDtypeStruct((depth, 2, 2, 2) + array.shape, array.dtype) for array in arrays
        ],
        in_specs=[pl.BlockSpec(memory_space=pl.ANY)] * count,
        out_specs=[pl.BlockSpec(memory_space=pl.ANY)] * count,
        scratch_shapes=[
            pltpu.SemaphoreType.DMA((count, copies)),
            pltpu.SemaphoreType.DMA((count, copies)),
            pltpu.SemaphoreType.DMA((count,)),
        ],
        compiler_params=pltpu.CompilerParams(
            collective_id=0, has_side_effects=True, vmem_limit_bytes=4 << 20
        ),
    )(*arrays)


def by_rows(full):
    return full.reshape(-1, full.shape[-1])


def by_columns(full):
    blocks = full.reshape((-1,) + full.shape[-2:])
    return jnp.transpose(blocks, (1, 0, 2)).reshape(blocks.shape[1], -1)


def gather_plain(w_query, w_key_value, w_out, w_gate, w_up, w_down):
    both = ("dp", "fsdp")
    return (
        jnp.concatenate(
            [
                lax.all_gather(w_query, both, axis=0, tiled=True),
                lax.all_gather(w_key_value, both, axis=0, tiled=True),
            ],
            axis=1,
        ),
        lax.all_gather(w_out, both, axis=1, tiled=True),
        lax.all_gather(w_gate, both, axis=0, tiled=True),
        lax.all_gather(w_up, both, axis=0, tiled=True),
        lax.all_gather(w_down, both, axis=1, tiled=True),
    )


def aligned(w_out):
    lanes = 128
    return (
        w_out.shape[1] % lanes == 0
        and lax.axis_size("fsdp") == 4
        and lax.axis_size("dp") % 4 == 0
    )


def gather_weights(w_query, w_key_value, w_out, w_gate, w_up, w_down):
    if not aligned(w_out):
        return gather_plain(w_query, w_key_value, w_out, w_gate, w_up, w_down)
    first = jnp.concatenate([w_query, w_key_value], axis=1)
    joint, out, gate, up, down = gather_all([first, w_out, w_gate, w_up, w_down])
    return by_rows(joint), by_columns(out), by_rows(gate), by_rows(up), by_columns(down)


def per_device(
    tokens, doc_ids, attn_gain, mlp_gain, w_query, w_key_value, w_out, w_gate, w_up, w_down
):
    rows = tokens.shape[0]
    rank = lax.axis_index(("dp", "fsdp"))
    normed = rms_scale(tokens, attn_gain)
    query_width = w_query.shape[1]
    pair_width = w_key_value.shape[1]
    head = pair_width // 2
    heads = query_width // head
    joint, out_full, gate_full, up_full, down_full = gather_weights(
        w_query, w_key_value, w_out, w_gate, w_up, w_down
    )
    raw = jnp.dot(normed, joint, preferred_element_type=jnp.float32)
    query_raw = raw[:, :query_width]
    pair_raw = raw[:, query_width:]
    position = rank * rows + jnp.arange(rows, dtype=jnp.int32)
    query = rotate(query_raw.reshape(rows, heads, head), position).astype(jnp.bfloat16)
    keys = rotate(pair_raw[:, None, :head], position)[:, 0, :].astype(jnp.bfloat16)
    values = pair_raw[:, head:].astype(jnp.bfloat16)
    own_pairs = jnp.concatenate([keys, values], axis=1)
    marks = doc_ids + 1
    amounts = [1] + [1 << level for level in range(SPAN.bit_length() - 1)]
    held_pairs = own_pairs
    held_marks = marks
    for order, amount in enumerate(amounts):
        moved_pairs, moved_marks = shifted((held_pairs, held_marks), ("dp", "fsdp"), amount)
        if order == 0:
            held_pairs = moved_pairs
            held_marks = moved_marks
        else:
            held_pairs = jnp.concatenate([moved_pairs, held_pairs], axis=0)
            held_marks = jnp.concatenate([moved_marks, held_marks], axis=0)
    every_pair = jnp.concatenate([held_pairs, own_pairs], axis=0)
    every_mark = jnp.concatenate([held_marks, marks], axis=0)
    mixed = attend_dense(
        query, every_pair[:, :head], every_pair[:, head:], every_mark, marks, held_pairs.shape[0]
    )
    attended = mixed.reshape(rows, query_width).astype(jnp.bfloat16)
    projected = jnp.dot(
        attended,
        out_full,
        preferred_element_type=jnp.float32,
    )
    resid = (tokens.astype(jnp.float32) + projected).astype(jnp.bfloat16)
    resid = lax.optimization_barrier(resid)
    normed_mlp = rms_scale(resid, mlp_gain)
    pieces = (gate_full, up_full)
    columns = normed_mlp
    gate = jnp.dot(columns, pieces[0], preferred_element_type=jnp.float32)
    up_value = jnp.dot(columns, pieces[1], preferred_element_type=jnp.float32)
    hidden = (jax.nn.silu(gate) * up_value).astype(jnp.bfloat16)
    down = jnp.dot(
        hidden,
        down_full,
        preferred_element_type=jnp.float32,
    )
    return (resid.astype(jnp.float32) + down).astype(jnp.bfloat16)


def solution(mesh):
    in_specs = (
        P(("dp", "fsdp"), None),
        P(("dp", "fsdp")),
        P(),
        P(),
        P(("dp", "fsdp"), None),
        P(("dp", "fsdp"), None),
        P(None, ("dp", "fsdp")),
        P(("dp", "fsdp"), None),
        P(("dp", "fsdp"), None),
        P(None, ("dp", "fsdp")),
    )
    out_specs = P(("dp", "fsdp"), None)
    return jax.shard_map(
        per_device, mesh=mesh, in_specs=in_specs, out_specs=out_specs, check_vma=False
    )
```

```python
import functools
import math

import jax
import jax.numpy as jnp
from jax import lax
from jax.experimental import pallas as pl
from jax.experimental.pallas import tpu as pltpu
from jax.sharding import PartitionSpec as P

SPAN = 4


EPS = 1e-05
THETA = 500000.0
NEGATIVE = -1e30


def shifted(array, axis, by):
    length = lax.axis_size(axis)
    pairs = [(i, i + by) for i in range(length) if 0 <= i + by < length]
    return lax.ppermute(array, axis, pairs)


def rms_scale(values, gain):
    wide = values.astype(jnp.float32)
    power = jnp.mean(wide * wide, axis=-1, keepdims=True)
    return (wide * lax.rsqrt(power + EPS) * gain).astype(jnp.bfloat16)


def rotate(values, position):
    head = values.shape[-1]
    half = head // 2
    freqs = THETA ** (-2.0 * jnp.arange(half, dtype=jnp.float32) / head)
    angle = position.astype(jnp.float32)[:, None, None] * freqs[None, None, :]
    cosine = jnp.cos(angle)
    sine = jnp.sin(angle)
    first = values[..., :half]
    second = values[..., half:]
    return jnp.concatenate(
        [first * cosine - second * sine, second * cosine + first * sine], axis=-1
    )


def head_scores(query, keys):
    return jnp.einsum("qhd,kd->hqk", query, keys, preferred_element_type=jnp.float32) / math.sqrt(
        query.shape[-1]
    )


def weigh_values(weights, values):
    return jnp.einsum(
        "hqk,kd->qhd", weights.astype(jnp.bfloat16), values, preferred_element_type=jnp.float32
    )


def attend_dense(query, keys, values, key_marks, marks, offset):
    scores = head_scores(query, keys)
    key_index = jnp.arange(keys.shape[0], dtype=jnp.int32)
    query_index = jnp.arange(query.shape[0], dtype=jnp.int32) + offset
    allowed = (key_marks[None, :] == marks[:, None]) & (key_index[None, :] <= query_index[:, None])
    scores = jnp.where(allowed[None, :, :], scores, NEGATIVE)
    peak = jnp.max(scores, axis=2, keepdims=True)
    weights = jnp.exp(scores - peak)
    totals = jnp.sum(weights, axis=2)
    return weigh_values(weights, values) / jnp.transpose(totals)[:, :, None]


MESH = pl.DeviceIdType.MESH


class Gather:
    def __init__(self, spot, own, full, send, recv, local, row):
        self.own, self.full = own, full
        self.send, self.recv, self.local, self.row = send, recv, local, row
        self.dp, self.fsdp, self.depth = spot
        self.z, self.y = self.dp // 2, self.dp % 2
        self.x, self.c = self.fsdp // 2, self.fsdp % 2
        self.right = (self.dp, (1 - self.x) * 2 + self.c)
        self.up = (self.z * 2 + 1 - self.y, self.fsdp)
        self.twin = (self.dp, self.x * 2 + 1 - self.c)
        self.base = self.depth - 1

    def peers(self):
        others = [
            (lax.rem(self.z + step, self.depth) * 2 + self.y, self.fsdp)
            for step in range(1, self.depth)
        ]
        return others + [self.right, self.up, self.twin]

    def copy(self, number, source, target, device):
        return pltpu.make_async_remote_copy(
            src_ref=source,
            dst_ref=target,
            send_sem=self.send.at[self.row, number],
            recv_sem=self.recv.at[self.row, number],
            device_id=device,
            device_id_type=MESH,
        )

    def column(self, y, x, number, device, c=None):
        c = self.c if c is None else c
        part = self.full.at[:, y, x, c]
        return self.copy(number, part, part, device)

    def half(self, y, x, which, number, device):
        middle = self.depth // 2
        part = self.full.at[pl.ds(which * middle, middle), y, x, self.c]
        return self.copy(number, part, part, device)

    def mine(self):
        return pltpu.make_async_copy(
            self.own, self.full.at[self.z, self.y, self.x, self.c], self.local.at[self.row]
        )

    def along(self, step):
        there = (lax.rem(self.z + step, self.depth) * 2 + self.y, self.fsdp)
        return self.copy(
            step - 1, self.own, self.full.at[self.z, self.y, self.x, self.c], there
        )

    def s0(self):
        self.mine().start()
        for step in range(1, self.depth):
            self.along(step).start()

    def s1(self):
        self.mine().wait()
        for step in range(1, self.depth):
            self.along(step).wait_recv()
        self.column(self.y, self.x, self.base, self.right).start()
        self.column(self.y, self.x, self.base + 1, self.up).start()
        self.column(self.y, self.x, self.base + 4, self.twin).start()

    def s2(self):
        self.column(self.y, self.x, self.base, self.right).wait_recv()
        self.column(self.y, self.x, self.base + 1, self.up).wait_recv()
        self.half(1 - self.y, self.x, 0, self.base + 2, self.right).start()
        self.half(self.y, 1 - self.x, 1, self.base + 3, self.up).start()
        self.column(self.y, 1 - self.x, self.base + 5, self.twin).start()
        self.column(1 - self.y, self.x, self.base + 6, self.twin).start()

    def s3(self):
        self.half(1 - self.y, self.x, 0, self.base + 2, self.right).wait_recv()
        self.half(self.y, 1 - self.x, 1, self.base + 3, self.up).wait_recv()
        self.column(1 - self.y, 1 - self.x, self.base + 7, self.twin).start()

    def s4(self):
        for step in range(1, self.depth):
            self.along(step).wait_send()
        self.column(self.y, self.x, self.base, self.right).wait_send()
        self.column(self.y, self.x, self.base + 1, self.up).wait_send()
        self.half(1 - self.y, self.x, 0, self.base + 2, self.right).wait_send()
        self.half(self.y, 1 - self.x, 1, self.base + 3, self.up).wait_send()
        self.column(self.y, self.x, self.base + 4, self.twin).wait()
        self.column(self.y, 1 - self.x, self.base + 5, self.twin).wait()
        self.column(1 - self.y, self.x, self.base + 6, self.twin).wait()
        self.column(1 - self.y, 1 - self.x, self.base + 7, self.twin).wait()


def greet(peers):
    barrier = pltpu.get_barrier_semaphore()
    for device in peers:
        pl.semaphore_signal(barrier, inc=1, device_id=device, device_id_type=MESH)
    pl.semaphore_wait(barrier, len(peers))


def normalize(source, gain_ref, target):
    step = 32

    @pl.loop(0, source.shape[0] // step)
    def _(index):
        part = pl.ds(pl.multiple_of(index * step, step), step)
        target[part, :] = rms_scale(source[part, :], gain_ref[...])


def tile_of(full, index, width):
    columns = pl.ds(pl.multiple_of(index * width, width), width)
    block = full[:, :, :, :, :, columns]
    return block.reshape(-1, width)


def pair_of(full, index):
    z, y, x = index // 4, lax.rem(index // 2, 2), lax.rem(index, 2)
    return jnp.concatenate([full[z, y, x, 0], full[z, y, x, 1]], axis=-1)


def turned(values, cosine, sine):
    half = values.shape[-1] // 2
    swapped = jnp.concatenate([values[:, half:], values[:, :half]], axis=-1)
    return (values * cosine + swapped * sine).astype(jnp.bfloat16)


def layer_kernel(depth, count, *refs):
    tokens, attn_gain, mlp_gain, cosine, sine, marks, mark_column = refs[:7]
    owns = refs[7 : 7 + count]
    out = refs[7 + count]
    rest = refs[8 + count :]
    fulls = rest[:count]
    (normed, raw, query, pairs, key_marks, attended, gates, hidden) = rest[count : count + 8]
    send, recv, local, halo_send, halo_recv = rest[count + 8 :]
    rows = tokens.shape[0]
    head = pairs.shape[-1] // 2
    heads = query.shape[-1] // head
    dp, fsdp = lax.axis_index("dp"), lax.axis_index("fsdp")
    lanes = 4
    rank = dp * lanes + fsdp
    total = depth * 2 * lanes

    def at(offset):
        there = lax.rem(rank + offset + total, total)
        return (there // lanes, lax.rem(there, lanes))

    spot = (dp, fsdp, depth)
    r = [Gather(spot, owns[i], fulls[i], send, recv, local, i) for i in range(count)]
    offsets = [sign * step for step in range(1, SPAN + 1) for sign in (1, -1)]
    greet(r[0].peers() + [at(offset) for offset in offsets])

    def halo(kind, step):
        source = (pairs.at[SPAN], marks)[kind]
        target = (pairs, key_marks)[kind].at[SPAN - step]
        return pltpu.make_async_remote_copy(
            src_ref=source,
            dst_ref=target,
            send_sem=halo_send.at[kind, step - 1],
            recv_sem=halo_recv.at[kind, step - 1],
            device_id=at(step),
            device_id_type=MESH,
        )

    for ride in r:
        ride.s0()
    for step in range(1, SPAN + 1):
        halo(1, step).start()
    normalize(tokens, attn_gain, normed)
    r[0].s1()
    r[1].s1()
    r[0].s2()
    r[2].s1()
    r[1].s2()
    r[0].s3()
    r[0].s4()

    wide = 256

    @pl.loop(0, raw.shape[1] // wide)
    def _(index):
        columns = pl.ds(pl.multiple_of(index * wide, wide), wide)
        raw[:, columns] = jnp.dot(
            normed[...], tile_of(fulls[0], index, wide), preferred_element_type=jnp.float32
        )

    base = heads * head
    pairs[SPAN, :, :head] = turned(raw[:, base : base + head], cosine[...], sine[...])
    pairs[SPAN, :, head:] = raw[:, base + head :].astype(jnp.bfloat16)
    for index in range(heads):
        cut = slice(index * head, (index + 1) * head)
        query[:, cut] = turned(raw[:, cut], cosine[...], sine[...])
    for step in range(1, SPAN + 1):
        halo(0, step).start()
    r[1].s3()
    r[3].s1()
    for step in range(1, SPAN + 1):
        halo(1, step).wait()
        halo(0, step).wait()

    part = 256
    scale = 1.0 / math.sqrt(head)
    reach = (SPAN + 1) * rows

    @pl.loop(0, (rows // part) * heads)
    def _(index):
        chunk, which = index // heads, lax.rem(index, heads)
        first = pl.multiple_of(chunk * part, part)
        here = pl.ds(first, part)
        columns = pl.ds(pl.multiple_of(which * head, head), head)
        keys = pairs[:, :, :head].reshape(reach, head)
        values = pairs[:, :, head:].reshape(reach, head)
        scores = lax.dot_general(
            query[here, columns], keys, (((1,), (1,)), ((), ())),
            preferred_element_type=jnp.float32,
        ) * scale
        seen = jnp.concatenate([key_marks[step] for step in range(SPAN)] + [marks[...]], axis=-1)
        key_index = lax.broadcasted_iota(jnp.int32, (1, reach), 1)
        query_index = lax.broadcasted_iota(jnp.int32, (part, 1), 0) + (first + SPAN * rows)
        inside = key_index >= (SPAN - rank) * rows
        seen = jnp.where(inside, seen, -1)
        allowed = (seen == mark_column[here, :]) & (key_index <= query_index)
        scores = jnp.where(allowed, scores, NEGATIVE)
        peak = jnp.max(scores, axis=1, keepdims=True)
        weights = jnp.exp(scores - peak)
        sums = jnp.sum(weights, axis=1, keepdims=True)
        mixed = jnp.dot(weights.astype(jnp.bfloat16), values, preferred_element_type=jnp.float32)
        attended[here, columns] = (mixed / sums).astype(jnp.bfloat16)

    r[2].s2()
    r[1].s4()
    pair_width = 2 * owns[1].shape[1]

    @pl.loop(0, out.shape[1] // pair_width)
    def _(index):
        columns = pl.ds(pl.multiple_of(index * pair_width, pair_width), pair_width)
        moved = jnp.dot(attended[...], pair_of(fulls[1], index), preferred_element_type=jnp.float32)
        out[:, columns] = (tokens[:, columns].astype(jnp.float32) + moved).astype(jnp.bfloat16)

    r[4].s1()
    normalize(out, mlp_gain, normed)
    r[3].s2()
    r[2].s3()
    r[2].s4()

    @pl.loop(0, gates.shape[1] // wide)
    def _(index):
        columns = pl.ds(pl.multiple_of(index * wide, wide), wide)
        gates[:, columns] = jnp.dot(
            normed[...], tile_of(fulls[2], index, wide), preferred_element_type=jnp.float32
        )

    r[4].s2()
    r[3].s3()
    r[3].s4()

    @pl.loop(0, gates.shape[1] // wide)
    def _(index):
        columns = pl.ds(pl.multiple_of(index * wide, wide), wide)
        up = jnp.dot(
            normed[...], tile_of(fulls[3], index, wide), preferred_element_type=jnp.float32
        )
        gate = gates[:, columns]
        hidden[:, columns] = (gate / (1.0 + jnp.exp(-gate)) * up).astype(jnp.bfloat16)

    r[4].s3()
    r[4].s4()

    @pl.loop(0, out.shape[1] // pair_width)
    def _(index):
        columns = pl.ds(pl.multiple_of(index * pair_width, pair_width), pair_width)
        moved = jnp.dot(hidden[...], pair_of(fulls[4], index), preferred_element_type=jnp.float32)
        out[:, columns] = (out[:, columns].astype(jnp.float32) + moved).astype(jnp.bfloat16)


def whole_layer(
    tokens, doc_ids, attn_gain, mlp_gain, w_query, w_key_value, w_out, w_gate, w_up, w_down
):
    depth = lax.axis_size("dp") // 2
    rows, model = tokens.shape
    query_width = w_query.shape[1]
    pair_width = w_key_value.shape[1]
    head = pair_width // 2
    rank = lax.axis_index(("dp", "fsdp"))
    position = rank * rows + jnp.arange(rows, dtype=jnp.int32)
    freqs = THETA ** (-2.0 * jnp.arange(head // 2, dtype=jnp.float32) / head)
    angle = position.astype(jnp.float32)[:, None] * freqs[None, :]
    cosine = jnp.cos(angle)
    sine = jnp.sin(angle)
    cosine = jnp.concatenate([cosine, cosine], axis=1)
    sine = jnp.concatenate([-sine, sine], axis=1)
    arrays = [jnp.concatenate([w_query, w_key_value], axis=1), w_out, w_gate, w_up, w_down]
    count = len(arrays)
    copies = depth - 1 + 8
    marks = doc_ids + 1
    vmem = pl.BlockSpec(memory_space=pltpu.VMEM)
    low = jnp.bfloat16
    return pl.pallas_call(
        functools.partial(layer_kernel, depth, count),
        out_shape=jax.ShapeDtypeStruct((rows, model), low),
        in_specs=[vmem] * 7 + [pl.BlockSpec(memory_space=pl.ANY)] * count,
        out_specs=vmem,
        scratch_shapes=[
            pltpu.VMEM((depth, 2, 2, 2) + array.shape, array.dtype) for array in arrays
        ]
        + [
            pltpu.VMEM((rows, model), low),
            pltpu.VMEM((rows, query_width + pair_width), jnp.float32),
            pltpu.VMEM((rows, query_width), low),
            pltpu.VMEM((SPAN + 1, rows, pair_width), low),
            pltpu.VMEM((SPAN, 1, rows), jnp.int32),
            pltpu.VMEM((rows, query_width), low),
            pltpu.VMEM((rows, w_gate.shape[1]), jnp.float32),
            pltpu.VMEM((rows, w_gate.shape[1]), low),
            pltpu.SemaphoreType.DMA((count, copies)),
            pltpu.SemaphoreType.DMA((count, copies)),
            pltpu.SemaphoreType.DMA((count,)),
            pltpu.SemaphoreType.DMA((2, SPAN)),
            pltpu.SemaphoreType.DMA((2, SPAN)),
        ],
        compiler_params=pltpu.CompilerParams(
            collective_id=0, has_side_effects=True, vmem_limit_bytes=67043328
        ),
    )(
        tokens,
        attn_gain[None, :],
        mlp_gain[None, :],
        cosine,
        sine,
        marks[None, :],
        marks[:, None],
        *arrays,
    )


def gather_plain(w_query, w_key_value, w_out, w_gate, w_up, w_down):
    both = ("dp", "fsdp")
    return (
        jnp.concatenate(
            [
                lax.all_gather(w_query, both, axis=0, tiled=True),
                lax.all_gather(w_key_value, both, axis=0, tiled=True),
            ],
            axis=1,
        ),
        lax.all_gather(w_out, both, axis=1, tiled=True),
        lax.all_gather(w_gate, both, axis=0, tiled=True),
        lax.all_gather(w_up, both, axis=0, tiled=True),
        lax.all_gather(w_down, both, axis=1, tiled=True),
    )


def aligned(w_out):
    lanes = 128
    return (
        w_out.shape[1] % lanes == 0
        and lax.axis_size("fsdp") == 4
        and lax.axis_size("dp") % 4 == 0
    )


def per_device(
    tokens, doc_ids, attn_gain, mlp_gain, w_query, w_key_value, w_out, w_gate, w_up, w_down
):
    if aligned(w_out):
        return whole_layer(
            tokens, doc_ids, attn_gain, mlp_gain, w_query, w_key_value, w_out, w_gate, w_up, w_down
        )
    rows = tokens.shape[0]
    rank = lax.axis_index(("dp", "fsdp"))
    normed = rms_scale(tokens, attn_gain)
    query_width = w_query.shape[1]
    pair_width = w_key_value.shape[1]
    head = pair_width // 2
    heads = query_width // head
    joint, out_full, gate_full, up_full, down_full = gather_plain(
        w_query, w_key_value, w_out, w_gate, w_up, w_down
    )
    raw = jnp.dot(normed, joint, preferred_element_type=jnp.float32)
    query_raw = raw[:, :query_width]
    pair_raw = raw[:, query_width:]
    position = rank * rows + jnp.arange(rows, dtype=jnp.int32)
    query = rotate(query_raw.reshape(rows, heads, head), position).astype(jnp.bfloat16)
    keys = rotate(pair_raw[:, None, :head], position)[:, 0, :].astype(jnp.bfloat16)
    values = pair_raw[:, head:].astype(jnp.bfloat16)
    own_pairs = jnp.concatenate([keys, values], axis=1)
    marks = doc_ids + 1
    amounts = [1] + [1 << level for level in range(SPAN.bit_length() - 1)]
    held_pairs = own_pairs
    held_marks = marks
    for order, amount in enumerate(amounts):
        moved_pairs, moved_marks = shifted((held_pairs, held_marks), ("dp", "fsdp"), amount)
        if order == 0:
            held_pairs = moved_pairs
            held_marks = moved_marks
        else:
            held_pairs = jnp.concatenate([moved_pairs, held_pairs], axis=0)
            held_marks = jnp.concatenate([moved_marks, held_marks], axis=0)
    every_pair = jnp.concatenate([held_pairs, own_pairs], axis=0)
    every_mark = jnp.concatenate([held_marks, marks], axis=0)
    mixed = attend_dense(
        query, every_pair[:, :head], every_pair[:, head:], every_mark, marks, held_pairs.shape[0]
    )
    attended = mixed.reshape(rows, query_width).astype(jnp.bfloat16)
    projected = jnp.dot(
        attended,
        out_full,
        preferred_element_type=jnp.float32,
    )
    resid = (tokens.astype(jnp.float32) + projected).astype(jnp.bfloat16)
    resid = lax.optimization_barrier(resid)
    normed_mlp = rms_scale(resid, mlp_gain)
    pieces = (gate_full, up_full)
    columns = normed_mlp
    gate = jnp.dot(columns, pieces[0], preferred_element_type=jnp.float32)
    up_value = jnp.dot(columns, pieces[1], preferred_element_type=jnp.float32)
    hidden = (jax.nn.silu(gate) * up_value).astype(jnp.bfloat16)
    down = jnp.dot(
        hidden,
        down_full,
        preferred_element_type=jnp.float32,
    )
    return (resid.astype(jnp.float32) + down).astype(jnp.bfloat16)


def solution(mesh):
    in_specs = (
        P(("dp", "fsdp"), None),
        P(("dp", "fsdp")),
        P(),
        P(),
        P(("dp", "fsdp"), None),
        P(("dp", "fsdp"), None),
        P(None, ("dp", "fsdp")),
        P(("dp", "fsdp"), None),
        P(("dp", "fsdp"), None),
        P(None, ("dp", "fsdp")),
    )
    out_specs = P(("dp", "fsdp"), None)
    return jax.shard_map(
        per_device, mesh=mesh, in_specs=in_specs, out_specs=out_specs, check_vma=False
    )
```

```python
import functools
import math

import jax
import jax.numpy as jnp
from jax import lax
from jax.experimental import pallas as pl
from jax.experimental.pallas import tpu as pltpu
from jax.sharding import PartitionSpec as P

SPAN = 4


EPS = 1e-05
THETA = 500000.0
NEGATIVE = -1e30


def shifted(array, axis, by):
    length = lax.axis_size(axis)
    pairs = [(i, i + by) for i in range(length) if 0 <= i + by < length]
    return lax.ppermute(array, axis, pairs)


def rms_scale(values, gain):
    wide = values.astype(jnp.float32)
    power = jnp.mean(wide * wide, axis=-1, keepdims=True)
    return (wide * lax.rsqrt(power + EPS) * gain).astype(jnp.bfloat16)


def rotate(values, position):
    head = values.shape[-1]
    half = head // 2
    freqs = THETA ** (-2.0 * jnp.arange(half, dtype=jnp.float32) / head)
    angle = position.astype(jnp.float32)[:, None, None] * freqs[None, None, :]
    cosine = jnp.cos(angle)
    sine = jnp.sin(angle)
    first = values[..., :half]
    second = values[..., half:]
    return jnp.concatenate(
        [first * cosine - second * sine, second * cosine + first * sine], axis=-1
    )


def head_scores(query, keys):
    return jnp.einsum("qhd,kd->hqk", query, keys, preferred_element_type=jnp.float32) / math.sqrt(
        query.shape[-1]
    )


def weigh_values(weights, values):
    return jnp.einsum(
        "hqk,kd->qhd", weights.astype(jnp.bfloat16), values, preferred_element_type=jnp.float32
    )


def attend_dense(query, keys, values, key_marks, marks, offset):
    scores = head_scores(query, keys)
    key_index = jnp.arange(keys.shape[0], dtype=jnp.int32)
    query_index = jnp.arange(query.shape[0], dtype=jnp.int32) + offset
    allowed = (key_marks[None, :] == marks[:, None]) & (key_index[None, :] <= query_index[:, None])
    scores = jnp.where(allowed[None, :, :], scores, NEGATIVE)
    peak = jnp.max(scores, axis=2, keepdims=True)
    weights = jnp.exp(scores - peak)
    totals = jnp.sum(weights, axis=2)
    return weigh_values(weights, values) / jnp.transpose(totals)[:, :, None]


MESH = pl.DeviceIdType.MESH


class Gather:
    def __init__(self, spot, own, full, send, recv, local, row):
        self.own, self.full = own, full
        self.send, self.recv, self.local, self.row = send, recv, local, row
        self.dp, self.fsdp, self.depth = spot
        self.z, self.y = self.dp // 2, self.dp % 2
        self.x, self.c = self.fsdp // 2, self.fsdp % 2
        self.right = (self.dp, (1 - self.x) * 2 + self.c)
        self.up = (self.z * 2 + 1 - self.y, self.fsdp)
        self.twin = (self.dp, self.x * 2 + 1 - self.c)
        self.base = self.depth - 1

    def peers(self):
        others = [
            (lax.rem(self.z + step, self.depth) * 2 + self.y, self.fsdp)
            for step in range(1, self.depth)
        ]
        return others + [self.right, self.up, self.twin]

    def copy(self, number, source, target, device):
        return pltpu.make_async_remote_copy(
            src_ref=source,
            dst_ref=target,
            send_sem=self.send.at[self.row, number],
            recv_sem=self.recv.at[self.row, number],
            device_id=device,
            device_id_type=MESH,
        )

    def column(self, y, x, number, device, c=None):
        c = self.c if c is None else c
        part = self.full.at[:, y, x, c]
        return self.copy(number, part, part, device)

    def half(self, y, x, which, number, device):
        middle = self.depth // 2
        part = self.full.at[pl.ds(which * middle, middle), y, x, self.c]
        return self.copy(number, part, part, device)

    def mine(self):
        return pltpu.make_async_copy(
            self.own, self.full.at[self.z, self.y, self.x, self.c], self.local.at[self.row]
        )

    def along(self, step):
        there = (lax.rem(self.z + step, self.depth) * 2 + self.y, self.fsdp)
        return self.copy(
            step - 1, self.own, self.full.at[self.z, self.y, self.x, self.c], there
        )

    def s0(self):
        self.mine().start()
        for step in range(1, self.depth):
            self.along(step).start()

    def s1(self):
        self.mine().wait()
        for step in range(1, self.depth):
            self.along(step).wait_recv()
        self.column(self.y, self.x, self.base, self.right).start()
        self.column(self.y, self.x, self.base + 1, self.up).start()
        self.column(self.y, self.x, self.base + 4, self.twin).start()

    def s2(self):
        self.column(self.y, self.x, self.base, self.right).wait_recv()
        self.column(self.y, self.x, self.base + 1, self.up).wait_recv()
        self.half(1 - self.y, self.x, 0, self.base + 2, self.right).start()
        self.half(self.y, 1 - self.x, 1, self.base + 3, self.up).start()
        self.column(self.y, 1 - self.x, self.base + 5, self.twin).start()
        self.column(1 - self.y, self.x, self.base + 6, self.twin).start()

    def s3(self):
        self.half(1 - self.y, self.x, 0, self.base + 2, self.right).wait_recv()
        self.half(self.y, 1 - self.x, 1, self.base + 3, self.up).wait_recv()
        self.column(1 - self.y, 1 - self.x, self.base + 7, self.twin).start()

    def s4(self):
        for step in range(1, self.depth):
            self.along(step).wait_send()
        self.column(self.y, self.x, self.base, self.right).wait_send()
        self.column(self.y, self.x, self.base + 1, self.up).wait_send()
        self.half(1 - self.y, self.x, 0, self.base + 2, self.right).wait_send()
        self.half(self.y, 1 - self.x, 1, self.base + 3, self.up).wait_send()
        self.column(self.y, self.x, self.base + 4, self.twin).wait()
        self.column(self.y, 1 - self.x, self.base + 5, self.twin).wait()
        self.column(1 - self.y, self.x, self.base + 6, self.twin).wait()
        self.column(1 - self.y, 1 - self.x, self.base + 7, self.twin).wait()


def greet(peers):
    barrier = pltpu.get_barrier_semaphore()
    for device in peers:
        pl.semaphore_signal(barrier, inc=1, device_id=device, device_id_type=MESH)
    pl.semaphore_wait(barrier, len(peers))


def normalize(source, gain_ref, target):
    step = 32

    @pl.loop(0, source.shape[0] // step)
    def _(index):
        part = pl.ds(pl.multiple_of(index * step, step), step)
        target[part, :] = rms_scale(source[part, :], gain_ref[...])


def tile_of(full, index, width):
    columns = pl.ds(pl.multiple_of(index * width, width), width)
    block = full[:, :, :, :, :, columns]
    return block.reshape(-1, width)


def pair_of(full, index):
    z, y, x = index // 4, lax.rem(index // 2, 2), lax.rem(index, 2)
    return jnp.concatenate([full[z, y, x, 0], full[z, y, x, 1]], axis=-1)


def turned(values, cosine, sine):
    half = values.shape[-1] // 2
    swapped = jnp.concatenate([values[:, half:], values[:, :half]], axis=-1)
    return (values * cosine + swapped * sine).astype(jnp.bfloat16)


def layer_kernel(depth, count, *refs):
    tokens, attn_gain, mlp_gain, cosine, sine, marks, mark_column = refs[:7]
    owns = refs[7 : 7 + count]
    out = refs[7 + count]
    rest = refs[8 + count :]
    fulls = rest[:count]
    (normed, raw, query, pairs, key_marks, attended, gates, hidden) = rest[count : count + 8]
    send, recv, local, halo_send, halo_recv = rest[count + 8 :]
    rows = tokens.shape[0]
    head = pairs.shape[-1] // 2
    heads = query.shape[-1] // head
    dp, fsdp = lax.axis_index("dp"), lax.axis_index("fsdp")
    lanes = 4
    rank = dp * lanes + fsdp
    total = depth * 2 * lanes

    def at(offset):
        there = lax.rem(rank + offset + total, total)
        return (there // lanes, lax.rem(there, lanes))

    spot = (dp, fsdp, depth)
    r = [Gather(spot, owns[i], fulls[i], send, recv, local, i) for i in range(count)]
    offsets = [sign * step for step in range(1, SPAN + 1) for sign in (1, -1)]
    greet(r[0].peers() + [at(offset) for offset in offsets])

    def halo(kind, step):
        source = (pairs.at[SPAN], marks)[kind]
        target = (pairs, key_marks)[kind].at[SPAN - step]
        return pltpu.make_async_remote_copy(
            src_ref=source,
            dst_ref=target,
            send_sem=halo_send.at[kind, step - 1],
            recv_sem=halo_recv.at[kind, step - 1],
            device_id=at(step),
            device_id_type=MESH,
        )

    r[0].s0()
    for step in range(1, SPAN + 1):
        halo(1, step).start()
    normalize(tokens, attn_gain, normed)
    r[0].s1()
    r[1].s0()
    r[1].s1()
    r[2].s0()
    r[0].s2()
    r[2].s1()
    r[3].s0()
    r[1].s2()
    r[0].s3()
    r[0].s4()

    wide = 256

    @pl.loop(0, raw.shape[1] // wide)
    def _(index):
        columns = pl.ds(pl.multiple_of(index * wide, wide), wide)
        raw[:, columns] = jnp.dot(
            normed[...], tile_of(fulls[0], index, wide), preferred_element_type=jnp.float32
        )

    base = heads * head
    pairs[SPAN, :, :head] = turned(raw[:, base : base + head], cosine[...], sine[...])
    pairs[SPAN, :, head:] = raw[:, base + head :].astype(jnp.bfloat16)
    for index in range(heads):
        cut = slice(index * head, (index + 1) * head)
        query[:, cut] = turned(raw[:, cut], cosine[...], sine[...])
    for step in range(1, SPAN + 1):
        halo(0, step).start()
    r[1].s3()
    r[3].s1()
    r[4].s0()
    for step in range(1, SPAN + 1):
        halo(1, step).wait()
        halo(0, step).wait()

    part = 256
    scale = 1.0 / math.sqrt(head)
    reach = (SPAN + 1) * rows

    @pl.loop(0, (rows // part) * heads)
    def _(index):
        chunk, which = index // heads, lax.rem(index, heads)
        first = pl.multiple_of(chunk * part, part)
        here = pl.ds(first, part)
        columns = pl.ds(pl.multiple_of(which * head, head), head)
        keys = pairs[:, :, :head].reshape(reach, head)
        values = pairs[:, :, head:].reshape(reach, head)
        scores = lax.dot_general(
            query[here, columns], keys, (((1,), (1,)), ((), ())),
            preferred_element_type=jnp.float32,
        ) * scale
        seen = jnp.concatenate([key_marks[step] for step in range(SPAN)] + [marks[...]], axis=-1)
        key_index = lax.broadcasted_iota(jnp.int32, (1, reach), 1)
        query_index = lax.broadcasted_iota(jnp.int32, (part, 1), 0) + (first + SPAN * rows)
        inside = key_index >= (SPAN - rank) * rows
        seen = jnp.where(inside, seen, -1)
        allowed = (seen == mark_column[here, :]) & (key_index <= query_index)
        scores = jnp.where(allowed, scores, NEGATIVE)
        peak = jnp.max(scores, axis=1, keepdims=True)
        weights = jnp.exp(scores - peak)
        sums = jnp.sum(weights, axis=1, keepdims=True)
        mixed = jnp.dot(weights.astype(jnp.bfloat16), values, preferred_element_type=jnp.float32)
        attended[here, columns] = (mixed / sums).astype(jnp.bfloat16)

    r[2].s2()
    r[1].s4()
    pair_width = 2 * owns[1].shape[1]

    @pl.loop(0, out.shape[1] // pair_width)
    def _(index):
        columns = pl.ds(pl.multiple_of(index * pair_width, pair_width), pair_width)
        moved = jnp.dot(attended[...], pair_of(fulls[1], index), preferred_element_type=jnp.float32)
        out[:, columns] = (tokens[:, columns].astype(jnp.float32) + moved).astype(jnp.bfloat16)

    r[4].s1()
    normalize(out, mlp_gain, normed)
    r[3].s2()
    r[2].s3()
    r[2].s4()

    @pl.loop(0, gates.shape[1] // wide)
    def _(index):
        columns = pl.ds(pl.multiple_of(index * wide, wide), wide)
        gates[:, columns] = jnp.dot(
            normed[...], tile_of(fulls[2], index, wide), preferred_element_type=jnp.float32
        )

    r[4].s2()
    r[3].s3()
    r[3].s4()

    @pl.loop(0, gates.shape[1] // wide)
    def _(index):
        columns = pl.ds(pl.multiple_of(index * wide, wide), wide)
        up = jnp.dot(
            normed[...], tile_of(fulls[3], index, wide), preferred_element_type=jnp.float32
        )
        gate = gates[:, columns]
        hidden[:, columns] = (gate / (1.0 + jnp.exp(-gate)) * up).astype(jnp.bfloat16)

    r[4].s3()
    r[4].s4()

    @pl.loop(0, out.shape[1] // pair_width)
    def _(index):
        columns = pl.ds(pl.multiple_of(index * pair_width, pair_width), pair_width)
        moved = jnp.dot(hidden[...], pair_of(fulls[4], index), preferred_element_type=jnp.float32)
        out[:, columns] = (out[:, columns].astype(jnp.float32) + moved).astype(jnp.bfloat16)


def whole_layer(
    tokens, doc_ids, attn_gain, mlp_gain, w_query, w_key_value, w_out, w_gate, w_up, w_down
):
    depth = lax.axis_size("dp") // 2
    rows, model = tokens.shape
    query_width = w_query.shape[1]
    pair_width = w_key_value.shape[1]
    head = pair_width // 2
    rank = lax.axis_index(("dp", "fsdp"))
    position = rank * rows + jnp.arange(rows, dtype=jnp.int32)
    freqs = THETA ** (-2.0 * jnp.arange(head // 2, dtype=jnp.float32) / head)
    angle = position.astype(jnp.float32)[:, None] * freqs[None, :]
    cosine = jnp.cos(angle)
    sine = jnp.sin(angle)
    cosine = jnp.concatenate([cosine, cosine], axis=1)
    sine = jnp.concatenate([-sine, sine], axis=1)
    arrays = [jnp.concatenate([w_query, w_key_value], axis=1), w_out, w_gate, w_up, w_down]
    count = len(arrays)
    copies = depth - 1 + 8
    marks = doc_ids + 1
    vmem = pl.BlockSpec(memory_space=pltpu.VMEM)
    low = jnp.bfloat16
    return pl.pallas_call(
        functools.partial(layer_kernel, depth, count),
        out_shape=jax.ShapeDtypeStruct((rows, model), low),
        in_specs=[vmem] * 7 + [pl.BlockSpec(memory_space=pl.ANY)] * count,
        out_specs=vmem,
        scratch_shapes=[
            pltpu.VMEM((depth, 2, 2, 2) + array.shape, array.dtype) for array in arrays
        ]
        + [
            pltpu.VMEM((rows, model), low),
            pltpu.VMEM((rows, query_width + pair_width), jnp.float32),
            pltpu.VMEM((rows, query_width), low),
            pltpu.VMEM((SPAN + 1, rows, pair_width), low),
            pltpu.VMEM((SPAN, 1, rows), jnp.int32),
            pltpu.VMEM((rows, query_width), low),
            pltpu.VMEM((rows, w_gate.shape[1]), jnp.float32),
            pltpu.VMEM((rows, w_gate.shape[1]), low),
            pltpu.SemaphoreType.DMA((count, copies)),
            pltpu.SemaphoreType.DMA((count, copies)),
            pltpu.SemaphoreType.DMA((count,)),
            pltpu.SemaphoreType.DMA((2, SPAN)),
            pltpu.SemaphoreType.DMA((2, SPAN)),
        ],
        compiler_params=pltpu.CompilerParams(
            collective_id=0, has_side_effects=True, vmem_limit_bytes=67043328
        ),
    )(
        tokens,
        attn_gain[None, :],
        mlp_gain[None, :],
        cosine,
        sine,
        marks[None, :],
        marks[:, None],
        *arrays,
    )


def gather_plain(w_query, w_key_value, w_out, w_gate, w_up, w_down):
    both = ("dp", "fsdp")
    return (
        jnp.concatenate(
            [
                lax.all_gather(w_query, both, axis=0, tiled=True),
                lax.all_gather(w_key_value, both, axis=0, tiled=True),
            ],
            axis=1,
        ),
        lax.all_gather(w_out, both, axis=1, tiled=True),
        lax.all_gather(w_gate, both, axis=0, tiled=True),
        lax.all_gather(w_up, both, axis=0, tiled=True),
        lax.all_gather(w_down, both, axis=1, tiled=True),
    )


def aligned(w_out):
    lanes = 128
    return (
        w_out.shape[1] % lanes == 0
        and lax.axis_size("fsdp") == 4
        and lax.axis_size("dp") % 4 == 0
    )


def per_device(
    tokens, doc_ids, attn_gain, mlp_gain, w_query, w_key_value, w_out, w_gate, w_up, w_down
):
    if aligned(w_out):
        return whole_layer(
            tokens, doc_ids, attn_gain, mlp_gain, w_query, w_key_value, w_out, w_gate, w_up, w_down
        )
    rows = tokens.shape[0]
    rank = lax.axis_index(("dp", "fsdp"))
    normed = rms_scale(tokens, attn_gain)
    query_width = w_query.shape[1]
    pair_width = w_key_value.shape[1]
    head = pair_width // 2
    heads = query_width // head
    joint, out_full, gate_full, up_full, down_full = gather_plain(
        w_query, w_key_value, w_out, w_gate, w_up, w_down
    )
    raw = jnp.dot(normed, joint, preferred_element_type=jnp.float32)
    query_raw = raw[:, :query_width]
    pair_raw = raw[:, query_width:]
    position = rank * rows + jnp.arange(rows, dtype=jnp.int32)
    query = rotate(query_raw.reshape(rows, heads, head), position).astype(jnp.bfloat16)
    keys = rotate(pair_raw[:, None, :head], position)[:, 0, :].astype(jnp.bfloat16)
    values = pair_raw[:, head:].astype(jnp.bfloat16)
    own_pairs = jnp.concatenate([keys, values], axis=1)
    marks = doc_ids + 1
    amounts = [1] + [1 << level for level in range(SPAN.bit_length() - 1)]
    held_pairs = own_pairs
    held_marks = marks
    for order, amount in enumerate(amounts):
        moved_pairs, moved_marks = shifted((held_pairs, held_marks), ("dp", "fsdp"), amount)
        if order == 0:
            held_pairs = moved_pairs
            held_marks = moved_marks
        else:
            held_pairs = jnp.concatenate([moved_pairs, held_pairs], axis=0)
            held_marks = jnp.concatenate([moved_marks, held_marks], axis=0)
    every_pair = jnp.concatenate([held_pairs, own_pairs], axis=0)
    every_mark = jnp.concatenate([held_marks, marks], axis=0)
    mixed = attend_dense(
        query, every_pair[:, :head], every_pair[:, head:], every_mark, marks, held_pairs.shape[0]
    )
    attended = mixed.reshape(rows, query_width).astype(jnp.bfloat16)
    projected = jnp.dot(
        attended,
        out_full,
        preferred_element_type=jnp.float32,
    )
    resid = (tokens.astype(jnp.float32) + projected).astype(jnp.bfloat16)
    resid = lax.optimization_barrier(resid)
    normed_mlp = rms_scale(resid, mlp_gain)
    pieces = (gate_full, up_full)
    columns = normed_mlp
    gate = jnp.dot(columns, pieces[0], preferred_element_type=jnp.float32)
    up_value = jnp.dot(columns, pieces[1], preferred_element_type=jnp.float32)
    hidden = (jax.nn.silu(gate) * up_value).astype(jnp.bfloat16)
    down = jnp.dot(
        hidden,
        down_full,
        preferred_element_type=jnp.float32,
    )
    return (resid.astype(jnp.float32) + down).astype(jnp.bfloat16)


def solution(mesh):
    in_specs = (
        P(("dp", "fsdp"), None),
        P(("dp", "fsdp")),
        P(),
        P(),
        P(("dp", "fsdp"), None),
        P(("dp", "fsdp"), None),
        P(None, ("dp", "fsdp")),
        P(("dp", "fsdp"), None),
        P(("dp", "fsdp"), None),
        P(None, ("dp", "fsdp")),
    )
    out_specs = P(("dp", "fsdp"), None)
    return jax.shard_map(
        per_device, mesh=mesh, in_specs=in_specs, out_specs=out_specs, check_vma=False
    )
```
